32 devices in a mesh: lat: 8 (over y, x, core), lon: 4 (over z).
Axes of the slice: x: 2, y: 2, z: 4, core: 2. Of those that a mesh axis runs over, the one named last changes fastest.
Arguments:
- right_side: float32 [128, 2560], P('lat', 'lon'), may hold values from -34 to 34
- first_guess: float32 [128, 2560], P('lat', 'lon'), may hold values from -3 to 3
- cell_mask: int32 [128, 2560], P('lat', 'lon'), may hold values 0 or 1
- cond_east: float32 [128, 2560], P('lat', 'lon'), may hold values from 0.5 to 2
- cond_north: float32 [128, 2560], P('lat', 'lon'), may hold values from 0.5 to 2
- surface: float32 [128, 2560], P('lat', 'lon'), may hold values from 0.02 to 0.5
- recycled: float32 [16, 128, 2560], P(None, 'lat', 'lon'), may hold values from -0.0031444706 to 0.0031444706
Outputs:
- solution: float32 [128, 2560], P('lat', 'lon')
- residual: float32 [128, 2560], P('lat', 'lon')
The draws below stay inside these ranges and needn't reach their ends.
All inputs are finite; a program needn't handle non-finite values. No bound on the sum of `cell_mask` on one device may be relied on, other than what follows from the above.
Results may differ from the reference program's by a relative error of at most 0.0003.
Values sent between devices are 32-bit elements; how exact they have to be, the bound alone decides.
A program may use at most 64 MiB of HBM per device.

```python
import math
import jax
import jax.numpy as jnp
from jax import lax

K = 16
ITERS = 3
NY = 128
NX = 2560


def basis_and_source(key):
    cells = NY * NX
    base = jax.random.fold_in(key, 7)
    key_phase, key_basis, key_weight, key_noise = jax.random.split(base, 4)
    phases = jax.random.uniform(key_phase, (2, K), jnp.float32, -3.1415927, 3.1415927)
    vector_index = jnp.arange(K)
    lat_wave = (vector_index % 4 + 1).astype(jnp.float32)
    lon_wave = (vector_index // 4 % 4).astype(jnp.float32)
    row_place = (jnp.arange(NY).astype(jnp.float32) + 0.5) / NY
    column_place = jnp.arange(NX).astype(jnp.float32) / NX
    lat_part = jnp.cos(3.1415927 * lat_wave[:, None] * row_place[None, :] + phases[0][:, None])
    lon_part = jnp.cos(6.2831853 * lon_wave[:, None] * column_place[None, :] + phases[1][:, None])
    pattern = lat_part[:, :, None] * lon_part[:, None, :]
    roughness = jnp.clip(jax.random.normal(key_basis, (K, NY, NX), jnp.float32), -4.0, 4.0)
    weights = jnp.clip(jax.random.normal(key_weight, (K,), jnp.float32), -2.5, 2.5) * 0.4
    noise = jnp.clip(jax.random.normal(key_noise, (NY, NX), jnp.float32), -4.0, 4.0)
    basis = pattern + 0.2 * roughness
    root = jnp.sqrt(jnp.float32(cells))
    source = noise + jnp.einsum('k,kyx->yx', weights, basis)
    return (basis / root, source)


def draw_recycled(key, part):
    return basis_and_source(key)[0].astype(jnp.float32)


def draw_right_side(key, part):
    return basis_and_source(key)[1].astype(jnp.float32)


def touch_ends(entries, own_key, low, high):
    longest = entries.shape.index(max(entries.shape))
    spots = []
    for shift in (0, 1):
        where = [jax.random.randint(jax.random.fold_in(own_key, axis), (), 0, length) for axis, length in enumerate(entries.shape)]
        where[longest] = (where[longest] + shift) % entries.shape[longest]
        spots.append(tuple(where))
    return entries.at[spots[0]].set(low).at[spots[1]].set(high)


def block_levels(rng, shape, cuts, low, top_value):
    gain = 1.0
    for axis_at, blocks in cuts:
        heights = jax.random.uniform(jax.random.fold_in(jax.random.fold_in(rng, 6), axis_at), (blocks,), jnp.float32, low / len(cuts), top_value / len(cuts))
        gain = gain * jnp.repeat(jnp.exp(heights), shape[axis_at] // blocks).reshape((-1,) + (1,) * (len(shape) - 1 - axis_at))
    return gain


def scatter_about(key, shape, width, bound, pieces=(), held_as=jnp.bfloat16):
    array = jax.random.normal(key, shape, jnp.float32) * width
    if len(pieces) > 0:
        array = block_levels(key, shape, pieces, -0.22, 0.18) * array
    return jnp.clip(array, min=-bound, max=bound).astype(held_as)


def setup_inputs(seed: int = 0) -> dict:
    key_of = jax.random.split(jax.random.key(seed), 8)
    right_side = draw_right_side(jax.random.fold_in(key_of[7], 71), 0)
    first_guess = scatter_about(key_of[1], (NY, NX), 0.5, 3.0, ((0, 8), (1, 4)), jnp.float32)
    cell_mask = touch_ends((jax.random.randint(key_of[2], (NY, NX), 0, 4) < 3).astype(jnp.int32), jax.random.fold_in(key_of[2], 1), 0, 1)
    cond_east = jnp.clip(jnp.exp(math.log(2.0) - 1.3862944 * jax.random.uniform(key_of[3], (NY, NX), jnp.float32) ** block_levels(key_of[3], (NY, NX), ((0, 8), (1, 4)), -0.2, 0.2)), 0.5, 2.0)
    cond_north = jnp.clip(jnp.exp(math.log(2.0) - 1.3862944 * jax.random.uniform(key_of[4], (NY, NX), jnp.float32) ** block_levels(key_of[4], (NY, NX), ((0, 8), (1, 4)), -0.2, 0.2)), 0.5, 2.0)
    surface = jnp.clip(jnp.exp(math.log(0.5) - 3.218876 * jax.random.uniform(key_of[5], (NY, NX), jnp.float32) ** block_levels(key_of[5], (NY, NX), ((0, 8), (1, 4)), -0.2, 0.2)), 0.02, 0.5)
    recycled = draw_recycled(jax.random.fold_in(key_of[7], 71), 0)
    return dict(right_side=right_side, first_guess=first_guess, cell_mask=cell_mask, cond_east=cond_east, cond_north=cond_north, surface=surface, recycled=recycled)


PRECISE = lax.Precision.HIGHEST

def neighbours(values):
    to_east = jnp.roll(values, -1, axis=-1)
    to_west = jnp.roll(values, 1, axis=-1)
    zero_row = jnp.zeros_like(values[..., :1, :])
    to_north = jnp.concatenate([values[..., 1:, :], zero_row], axis=-2)
    to_south = jnp.concatenate([zero_row, values[..., :-1, :]], axis=-2)
    return (to_east, to_west, to_north, to_south)

def faces(cell_mask, cond_east, cond_north, surface):
    wet_cells = cell_mask.astype(jnp.float32)
    wet_east = cond_east * wet_cells
    wet_north = cond_north * wet_cells
    ocean_e, ocean_w, ocean_n, ocean_s = neighbours(wet_cells)
    k_east = wet_east * ocean_e
    k_west = neighbours(wet_east)[1] * wet_cells
    k_north = wet_north * ocean_n
    k_south = neighbours(wet_north)[3] * wet_cells
    centre = surface * wet_cells + k_east + k_west + k_north + k_south + (1.0 - wet_cells)
    return (centre, k_east, k_west, k_north, k_south)

def operate(values, coeffs):
    centre, k_east, k_west, k_north, k_south = coeffs
    to_east, to_west, to_north, to_south = neighbours(values)
    return centre * values - (k_east * to_east + k_west * to_west + k_north * to_north + k_south * to_south)

def solve_small(factor, target):
    return jax.scipy.linalg.cho_solve((factor, True), target)

def reference(right_side, first_guess, cell_mask, cond_east, cond_north, surface, recycled):
    coeffs = faces(cell_mask, cond_east, cond_north, surface)
    basis_image = lax.map(lambda vector: operate(vector, coeffs), recycled)
    start_res = right_side - operate(first_guess, coeffs)
    gram = jnp.einsum('kyx,lyx->kl', recycled, basis_image, precision=PRECISE)
    start = jnp.einsum('kyx,yx->k', recycled, start_res, precision=PRECISE)
    factor = jnp.linalg.cholesky(0.5 * (gram + gram.T))
    coarse = solve_small(factor, start)
    solution = first_guess + jnp.einsum('kyx,k->yx', recycled, coarse, precision=PRECISE)
    residual = start_res - jnp.einsum('kyx,k->yx', basis_image, coarse, precision=PRECISE)
    direction = residual
    dir_image = residual
    curv = jnp.float32(1.0)
    prev_norm = jnp.float32(1.0)
    for turn_index in range(ITERS):
        image_res = operate(residual, coeffs)
        res_norm = jnp.sum(residual * residual)
        res_image = jnp.sum(residual * image_res)
        defl = jnp.einsum('kyx,yx->k', basis_image, residual, precision=PRECISE)
        coef = solve_small(factor, defl)
        along_basis = jnp.einsum('kyx,k->yx', recycled, coef, precision=PRECISE)
        along_image = jnp.einsum('kyx,k->yx', basis_image, coef, precision=PRECISE)
        if turn_index == 0:
            direction = residual - along_basis
            dir_image = image_res - along_image
            curv = res_image - jnp.sum(coef * defl)
        else:
            ratio = res_norm / prev_norm
            direction = residual - along_basis + ratio * direction
            dir_image = image_res - along_image + ratio * dir_image
            curv = res_image - jnp.sum(coef * defl) - ratio * ratio * curv
        step_len = res_norm / curv
        solution = solution + step_len * direction
        residual = residual - step_len * dir_image
        prev_norm = res_norm
    return (solution, residual)
```

```python
import functools

import jax
import jax.numpy as jnp
from jax import lax
from jax.experimental import pallas as pl
from jax.experimental.pallas import tpu as pltpu
from jax.sharding import PartitionSpec as P

MESH = pl.DeviceIdType.MESH
ITERS = 3
H = 4
F32 = jnp.float32
THETA = 5.5


def kernel(
    n_lat, n_lon, K, R, C,
    b_hbm, x0_hbm, mask_hbm, ce_hbm, cn_hbm, surf_hbm, w_hbm,
    x_out, r_out,
    stage_w, st_b, st_x0, st_mask, st_ce, st_cn, st_surf,
    ext, zbuf, coef, pack, packs_in, part, red1, red2,
    load_sem, send_sem, recv_sem, s1_send, s1_recv, s2_send, s2_recv,
):
    lat = lax.axis_index("lat")
    lon = lax.axis_index("lon")
    RE = R + 2 * H
    CE = C + 128
    S = 24
    NL = H + 1
    Z = NL * K + 16
    has_n = lat < n_lat - 1
    has_s = lat > 0
    east = lax.rem(lon + 1, n_lon)
    west = lax.rem(lon + n_lon - 1, n_lon)

    loads = []
    pairs = tuple(
        (w_hbm.at[:, pl.ds(128 * t, 128)], stage_w.at[t]) for t in range(C // 128)
    ) + (
        (b_hbm, st_b), (x0_hbm, st_x0), (mask_hbm, st_mask),
        (ce_hbm, st_ce), (cn_hbm, st_cn), (surf_hbm, st_surf),
    )
    for i, (src, dst) in enumerate(pairs):
        c = pltpu.make_async_copy(src, dst, load_sem.at[i])
        c.start()
        loads.append(c)

    barrier = pltpu.get_barrier_semaphore()

    def greet_lat(d, _):
        pl.semaphore_signal(barrier, inc=1, device_id=(lax.rem(lat + d, n_lat), lon), device_id_type=MESH)
        return 0

    def greet_lon(d, _):
        pl.semaphore_signal(barrier, inc=1, device_id=(lat, lax.rem(lon + d, n_lon)), device_id_type=MESH)
        return 0

    lax.fori_loop(1, n_lat, greet_lat, 0)
    lax.fori_loop(1, n_lon, greet_lon, 0)

    @pl.when(has_n)
    def _():
        for t in (east, west):
            pl.semaphore_signal(barrier, inc=1, device_id=(lat + 1, t), device_id_type=MESH)

    @pl.when(has_s)
    def _():
        for t in (east, west):
            pl.semaphore_signal(barrier, inc=1, device_id=(lat - 1, t), device_id_type=MESH)

    for c in loads:
        c.wait()

    for t in range(C // 128):
        ln = pl.ds(128 * t, 128)
        for y in range(R):
            v = stage_w[t, pl.ds(y, K, stride=R), :]
            ext[t, pl.ds(S * y, K), :] = v
            zbuf[t, pl.ds(Z * y, K), :] = v
        fields = (
            st_x0[:, ln], st_b[:, ln], st_mask[:, ln].astype(F32), st_ce[:, ln], st_cn[:, ln], st_surf[:, ln],
        )
        for f, v in enumerate(fields):
            ext[t, pl.ds(K + f, R, stride=S), :] = v
        for f in range(K + 6, S):
            ext[t, pl.ds(f, R, stride=S), :] = jnp.zeros((R, 128), F32)

    lane_s = lax.broadcasted_iota(jnp.int32, (S, 128), 1)
    acc = jnp.zeros((S, 128), F32)
    half = 64
    for y in range(R):
        lo = ext[0, pl.ds(S * y, S), :]
        hi = ext[C // 128 - 1, pl.ds(S * y, S), :]
        a0 = H * y
        if a0:
            lo = pltpu.roll(lo, a0, 1)
        hi = pltpu.roll(hi, (half + a0 + H - 128) % 128, 1)
        acc = jnp.where((lane_s >= a0) & (lane_s < a0 + H), lo, acc)
        acc = jnp.where((lane_s >= half + a0) & (lane_s < half + a0 + H), hi, acc)
    pack[...] = acc

    side = has_n.astype(jnp.int32) + has_s.astype(jnp.int32)
    pl.semaphore_wait(barrier, (n_lat - 1) + (n_lon - 1) + 2 * side)

    own = pl.ds(0, C // 128)

    def copy(src, dst, i, dev):
        return pltpu.make_async_remote_copy(
            src_ref=src, dst_ref=dst, send_sem=send_sem.at[i], recv_sem=recv_sem.at[i],
            device_id=dev, device_id_type=MESH,
        )

    to_n = (
        copy(ext.at[own, pl.ds(S * (R - H), S * H)], ext.at[own, pl.ds(S * (R + H), S * H)], 0, (lat + 1, lon)),
        copy(pack, packs_in.at[2], 4, (lat + 1, east)),
        copy(pack, packs_in.at[3], 5, (lat + 1, west)),
    )
    to_s = (
        copy(ext.at[own, pl.ds(0, S * H)], ext.at[own, pl.ds(S * R, S * H)], 1, (lat - 1, lon)),
        copy(pack, packs_in.at[4], 6, (lat - 1, east)),
        copy(pack, packs_in.at[5], 7, (lat - 1, west)),
    )
    to_e = copy(pack, packs_in.at[0], 2, (lat, east))
    to_w = copy(pack, packs_in.at[1], 3, (lat, west))

    to_e.start()
    to_w.start()

    @pl.when(has_n)
    def _():
        for c in to_n:
            c.start()

    @pl.when(has_s)
    def _():
        for c in to_s:
            c.start()

    to_e.wait()
    to_w.wait()

    @pl.when(has_n)
    def _():
        for c in to_n:
            c.wait_send()
        for c in to_s:
            c.wait_recv()

    @pl.when(has_s)
    def _():
        for c in to_s:
            c.wait_send()
        for c in to_n:
            c.wait_recv()

    @pl.when(jnp.logical_not(has_n))
    def _():
        ext[:, pl.ds(S * R, S * H), :] = jnp.zeros((CE // 128, S * H, 128), F32)

    @pl.when(jnp.logical_not(has_s))
    def _():
        ext[:, pl.ds(S * (R + H), S * H), :] = jnp.zeros((CE // 128, S * H, 128), F32)

    def unpack(y_ext, y_src, west_slot, east_slot, keep):
        from_e = packs_in[east_slot]
        from_w = packs_in[west_slot]
        e = pltpu.roll(from_e, (128 - H * y_src) % 128, 1) if y_src else from_e
        w = pltpu.roll(from_w, (128 - H - half - H * y_src) % 128, 1)
        v = jnp.where(lane_s < H, e, jnp.where(lane_s >= 128 - H, w, 0.0))
        if keep is not None:
            v = jnp.where(keep, v, 0.0)
        ext[C // 128, pl.ds(S * y_ext, S), :] = v

    for y in range(R):
        unpack(y, y, 0, 1, None)
    for y in range(H):
        unpack(R + y, y, 4, 5, has_n)
        unpack(R + H + y, R - H + y, 2, 3, has_s)

    def field(f):
        return jnp.concatenate(
            [ext[t, pl.ds(K + f, RE, stride=S), :] for t in range(CE // 128)], axis=1
        )

    def e_of(v):
        return pltpu.roll(v, CE - 1, 1)

    def w_of(v):
        return pltpu.roll(v, 1, 1)

    def n_of(v):
        return pltpu.roll(v, RE - 1, 0)

    def s_of(v):
        return pltpu.roll(v, 1, 0)

    x0 = field(0)
    rhs = field(1)
    wet = field(2)
    cew = field(3) * wet
    cnw = field(4) * wet
    k_e = cew * e_of(wet)
    k_w = w_of(cew) * wet
    k_n = cnw * n_of(wet)
    k_s = s_of(cnw) * wet
    centre = field(5) * wet + k_e + k_w + k_n + k_s + (1.0 - wet)
    for i, v in enumerate((centre, k_e, k_w, k_n, k_s)):
        coef[i] = v

    def operate(v):
        return centre * v - (k_e * e_of(v) + k_w * w_of(v) + k_n * n_of(v) + k_s * s_of(v))

    s_fam = [rhs - operate(x0)]
    for _ in range(ITERS):
        s_fam.append(operate(s_fam[-1]) - THETA * s_fam[-1])
    for t in range(C // 128):
        ln = pl.ds(128 * t, 128)
        for i, v in enumerate(s_fam):
            p = v[:R, 128 * t:128 * t + 128]
            p_hi = p.astype(jnp.bfloat16).astype(F32)
            zbuf[t, pl.ds(NL * K + i, R, stride=Z), :] = p_hi
            zbuf[t, pl.ds(NL * K + 4 + i, R, stride=Z), :] = p - p_hi
        for i in range(8, 16):
            zbuf[t, pl.ds(NL * K + i, R, stride=Z), :] = jnp.zeros((R, 128), F32)

    def rows(ref, level, y):
        start = S * y if level == 0 else Z * y + level * K
        at = pl.ds(pl.multiple_of(start, 8), K)
        return jnp.concatenate([ref[t, at, :] for t in range(CE // 128)], axis=1)

    for level in range(1, NL):
        h = NL - 1 - level
        src = ext if level == 1 else zbuf

        def body(t, _, level=level, h=h, src=src):
            y = lax.rem(t + (RE - h), RE)
            yn = lax.rem(y + 1, RE)
            ys = lax.rem(y + RE - 1, RE)
            v = rows(src, level - 1, y)
            vn = rows(src, level - 1, yn)
            vs = rows(src, level - 1, ys)

            def kk(i):
                return coef[i, pl.ds(y, 1), :]

            diag = kk(0) if level == 1 else kk(0) - THETA
            out = diag * v - (kk(1) * e_of(v) + kk(2) * w_of(v) + kk(3) * vn + kk(4) * vs)
            at = pl.ds(pl.multiple_of(Z * y + level * K, 8), K)
            for u in range(CE // 128):
                zbuf[u, at, :] = out[:, 128 * u:128 * u + 128]
            return 0

        lax.fori_loop(0, R + 2 * h, body, 0)

    def gram_step(t, total):
        z = jnp.concatenate(
            [
                zbuf[q, pl.ds(pl.multiple_of(Z * (2 * t + u), 8), Z), :]
                for u in range(2) for q in range(C // 128)
            ],
            axis=1,
        )
        hi = z.astype(jnp.bfloat16)
        lo = (z - hi.astype(F32)).astype(jnp.bfloat16)
        both = jnp.concatenate([hi, lo[:NL * K]], axis=0)
        return total + lax.dot_general(
            both, both, (((1,), (1,)), ((), ())), preferred_element_type=F32
        )

    G = lax.fori_loop(0, R // 2, gram_step, jnp.zeros((Z + NL * K, Z + NL * K), F32))
    zl = jnp.zeros((Z + NL * K, 256 - Z - NL * K), F32)
    G = jnp.concatenate([G, zl], axis=1)
    GL = pltpu.roll(G, 256 - Z, 1)[:, :128]
    G = G[:, :128]

    lane = lax.broadcasted_iota(jnp.int32, (K, 128), 1)
    sub = lax.broadcasted_iota(jnp.int32, (K, 128), 0)

    def moved(v, src, dst):
        s = (dst - src) % 128
        return pltpu.roll(v, s, 1) if s else v

    SB = NL * K
    NM = 2 * ITERS + 1
    AB = NM * K
    P_ = jnp.zeros((K, 128), F32)
    for m in range(1, NM + 1):
        i = m // 2
        j = m - i
        hh = G[i * K:(i + 1) * K] + G[Z + i * K:Z + (i + 1) * K]
        hl = GL[i * K:(i + 1) * K] + GL[Z + i * K:Z + (i + 1) * K]
        dst = (m - 1) * K
        v = moved(hh + hl, j * K, dst)
        P_ = jnp.where((lane >= dst) & (lane < dst + K), v, P_)
    for m in range(NM):
        j = m // 2
        i = m - j
        hh = G[i * K:(i + 1) * K] + G[Z + i * K:Z + (i + 1) * K]
        v = moved(hh, SB + j, AB + m) + moved(hh, SB + 4 + j, AB + m)
        P_ = jnp.where(lane == AB + m, v, P_)
    SL = AB + NM
    for m in range(2 * ITERS):
        i = m // 2
        j = m - i
        g = G[SB:SB + 8]
        v = moved(g, SB + j, SL) + moved(g, SB + 4 + j, SL)
        P_ = jnp.where((lane == SL) & (sub == m), v[i:i + 1] + v[4 + i:5 + i], P_)
    part[...] = P_

    def exchange(src, slots, send, recv, n, me, dev):
        def desc(d):
            return pltpu.make_async_remote_copy(
                src_ref=src, dst_ref=slots.at[me], send_sem=send.at[d], recv_sem=recv.at[me],
                device_id=dev(lax.rem(me + d, n)), device_id_type=MESH,
            )

        def from_slot(d):
            slot = lax.rem(me + d, n)
            return pltpu.make_async_remote_copy(
                src_ref=src, dst_ref=slots.at[slot], send_sem=send.at[d], recv_sem=recv.at[slot],
                device_id=dev(slot), device_id_type=MESH,
            )

        def start(d, _):
            desc(d).start()
            return 0

        def finish(d, _):
            desc(d).wait_send()
            from_slot(d).wait_recv()
            return 0

        lax.fori_loop(1, n, start, 0)
        slots[me] = src[...]
        lax.fori_loop(1, n, finish, 0)
        return lax.fori_loop(0, n, lambda d, t: t + slots[d], jnp.zeros((K, 128), F32))

    part[...] = exchange(part, red1, s1_send, s1_recv, n_lat, lat, lambda o: (o, lon))
    M = exchange(part, red2, s2_send, s2_recv, n_lon, lon, lambda o: (lat, o))

    MT = M.T
    sym = M
    for m in range(NM):
        t = MT[m * K:(m + 1) * K]
        t = jnp.concatenate([t, jnp.zeros((K, 128 - K), F32)], axis=1)
        t = moved(t, 0, m * K)
        sym = jnp.where((lane >= m * K) & (lane < (m + 1) * K), 0.5 * (M + t), sym)

    Q = sym
    for k in range(K):
        column = jnp.broadcast_to(Q[:, k:k + 1], (K, 128))
        pivot = column[k:k + 1]
        unit = (sub == k).astype(F32)
        Q = jnp.where(lane == k, unit, Q)
        Q = Q - (column - unit) * (Q[k:k + 1] / pivot)

    def col(v, m):
        return jnp.sum(jnp.where(lane == (m - 1) * K + sub, v, 0.0), axis=1, keepdims=True)

    def row_of(v):
        return jnp.sum(Q * v, axis=0, keepdims=True)

    def tiled(v):
        return jnp.sum(jnp.where(lax.rem(lane, K) == sub, v, 0.0), axis=0, keepdims=True)

    lane8 = lax.broadcasted_iota(jnp.int32, (8, 128), 1)
    sub8 = lax.broadcasted_iota(jnp.int32, (8, 128), 0)
    seg_mask = lane8 // K == sub8

    def seg_dots(t, v):
        d = jnp.sum(jnp.where(seg_mask, t * v, 0.0), axis=1, keepdims=True)
        return lambda m: d[m - 1:m]

    a = [sym[:, AB + m:AB + m + 1] for m in range(NM)]
    sigma = [M[m:m + 1, SL:SL + 1] for m in range(2 * ITERS)]

    U = row_of(a[0])
    c = col(U, 1)
    cu = seg_dots(tiled(c), U)
    b = [None] + [a[m] - col(U, m + 1) for m in range(1, 4)]
    sg = [sigma[m] - 2.0 * U[:, AB + m + 1:AB + m + 2] + cu(m + 2) for m in range(2 * ITERS)]

    def products(v):
        r = row_of(v)
        q = col(r, 1)
        qt = tiled(q)
        qu = seg_dots(qt, U)
        qb = lambda m: r[:, AB + m:AB + m + 1] - qu(m + 1)
        return r, q, qt, qb

    zero = jnp.zeros((1, 1), F32)

    def norm2(f, gx, gy, gz, e):
        t = gx * gx * q0v(2 + e)
        for i in range(len(f)):
            for k in range(len(f)):
                t = t + f[i] * f[k] * sg[i + k + e]
            t = t + 2.0 * f[i] * gx * q0b(i + 1 + e)
            if gz is not None:
                t = t + 2.0 * f[i] * (gy * q1b(i + 1 + e) + gz * q0b(i + 2 + e))
        if gz is not None:
            t = t + 2.0 * gx * gy * q1v(2 + e) + gy * gy * q1w(2 + e)
            t = t + 2.0 * gz * (gx * q0v(3 + e) + gy * q1v(3 + e)) + gz * gz * q0v(4 + e)
        return t

    V, q0, q0t, q0b = products(b[1])
    q0v = seg_dots(q0t, V)
    v2, v3 = col(V, 2), col(V, 3)
    rn0 = sg[0]
    rz0 = sg[1] + THETA * rn0
    curv0 = rz0 - q0b(1)
    al0 = rn0 / curv0
    f = [1.0 - al0 * THETA, -al0]
    d1 = f[0] * b[1] + f[1] * b[2] + al0 * v2
    Wr, q1, q1t, q1b = products(d1)
    q1v = seg_dots(q1t, V)
    q1w = seg_dots(q1t, Wr)
    w2 = col(Wr, 2)
    rn1 = norm2(f, al0, None, None, 0)
    rz1 = norm2(f, al0, None, None, 1) + THETA * rn1
    be1 = rn1 / rn0
    curv1 = rz1 - jnp.sum(q1 * d1, axis=0, keepdims=True) - be1 * be1 * curv0
    al1 = rn1 / curv1
    gx = al0 - al1 * (THETA * al0 - be1)
    gy = al1
    gz = -al1 * al0
    f = [
        f[0] - al1 * THETA * (f[0] + be1),
        f[1] - al1 * (f[0] + THETA * f[1] + be1),
        -al1 * f[1],
    ]
    d2 = f[0] * b[1] + f[1] * b[2] + f[2] * b[3] + gx * v2 + gy * w2 + gz * v3
    rn2 = norm2(f, gx, gy, gz, 0)
    rz2 = norm2(f, gx, gy, gz, 1) + THETA * rn2
    be2 = rn2 / rn1
    q2 = col(row_of(d2), 1)
    curv2 = rz2 - jnp.sum(q2 * d2, axis=0, keepdims=True) - be2 * be2 * curv1
    al2 = rn2 / curv2

    zc = jnp.zeros((K, 1), F32)

    def combine(x, scale, y):
        n = max(len(x[0]), len(y[0]))
        pad = lambda l, z0, k: list(l) + [z0] * (k - len(l))
        fx, fy = pad(x[0], zero, n), pad(y[0], zero, n)
        m = max(len(x[1]), len(y[1]))
        gx_, gy_ = pad(x[1], zc, m), pad(y[1], zc, m)
        return [p + scale * q for p, q in zip(fx, fy)], [p + scale * q for p, q in zip(gx_, gy_)]

    def shift(x):
        fs = [zero] + x[0]
        gs = [zc] + x[1]
        for i, e in enumerate(x[0]):
            fs[i] = fs[i] + THETA * e
        for i, e in enumerate(x[1]):
            if i:
                gs[i] = gs[i] + THETA * e
        return fs, gs

    one = jnp.ones((1, 1), F32)
    r = ([one], [zc, -c])
    x = ([zero], [c])
    p = combine(r, -one, ([zero], [q0]))
    x = combine(x, al0, p)
    r = combine(r, -al0, shift(p))
    p = combine(combine(r, -one, ([zero], [q1])), be1, p)
    x = combine(x, al1, p)
    r = combine(r, -al1, shift(p))
    p = combine(combine(r, -one, ([zero], [q2])), be2, p)
    x = combine(x, al2, p)
    r = combine(r, -al2, shift(p))

    def column_of(v):
        fs = list(v[0]) + [zero] * (4 - len(v[0]))
        gs = list(v[1]) + [zc] * (NL - len(v[1]))
        s8 = lax.broadcasted_iota(jnp.int32, (16, 128), 0)
        tail = jnp.zeros((16, 128), F32)
        for i, e in enumerate(fs):
            tail = jnp.where((s8 == i) | (s8 == 4 + i), e, tail)
        return [jnp.broadcast_to(g, (K, 128)) for g in gs] + [tail]

    cx = column_of(x)
    cr = column_of(r)
    for y in range(R):
        for t in range(C // 128):
            ln = pl.ds(128 * t, 128)
            tx = jnp.zeros((K, 128), F32)
            tr = jnp.zeros((K, 128), F32)
            for i in range(NL + 1):
                z = zbuf[t, pl.ds(Z * y + i * K, K), :]
                tx = tx + cx[i] * z
                tr = tr + cr[i] * z
            x_out[pl.ds(y, 1), ln] = st_x0[pl.ds(y, 1), ln] + jnp.sum(tx, axis=0, keepdims=True)
            r_out[pl.ds(y, 1), ln] = jnp.sum(tr, axis=0, keepdims=True)


def solution(mesh):
    n_lat, n_lon = mesh.shape["lat"], mesh.shape["lon"]

    def shards(right_side, first_guess, cell_mask, cond_east, cond_north, surface, recycled):
        K, R, C = recycled.shape
        RE, CE, S, Z = R + 2 * H, C + 128, 24, (H + 1) * K + 16
        block = jax.ShapeDtypeStruct((R, C), F32)
        vm = pltpu.VMEM
        dma = pltpu.SemaphoreType.DMA
        return pl.pallas_call(
            functools.partial(kernel, n_lat, n_lon, K, R, C),
            out_shape=(block, block),
            in_specs=[pl.BlockSpec(memory_space=pl.ANY)] * 7,
            out_specs=(pl.BlockSpec(memory_space=pltpu.VMEM),) * 2,
            scratch_shapes=[
                vm((C // 128, K * R, 128), F32),
                vm((R, C), F32), vm((R, C), F32), vm((R, C), jnp.int32),
                vm((R, C), F32), vm((R, C), F32), vm((R, C), F32),
                vm((CE // 128, S * RE, 128), F32),
                vm((CE // 128, Z * RE, 128), F32),
                vm((5, RE, CE), F32),
                vm((S, 128), F32),
                vm((6, S, 128), F32),
                vm((K, 128), F32),
                vm((n_lat, K, 128), F32),
                vm((n_lon, K, 128), F32),
                dma((6 + C // 128,)), dma((8,)), dma((8,)),
                dma((n_lat,)), dma((n_lat,)), dma((n_lon,)), dma((n_lon,)),
            ],
            compiler_params=pltpu.CompilerParams(
                collective_id=0, has_side_effects=True, vmem_limit_bytes=48 * 1024 * 1024
            ),
        )(
            right_side, first_guess, cell_mask, cond_east, cond_north, surface,
            recycled.reshape(K * R, C),
        )

    spec = P("lat", "lon")
    return jax.shard_map(
        shards,
        mesh=mesh,
        in_specs=(spec,) * 6 + (P(None, "lat", "lon"),),
        out_specs=(spec, spec),
        check_vma=False,
    )
```

```python
import functools

import jax
import jax.numpy as jnp
from jax import lax
from jax.experimental import pallas as pl
from jax.experimental.pallas import tpu as pltpu
from jax.sharding import PartitionSpec as P

MESH = pl.DeviceIdType.MESH
ITERS = 3
H = 4
F32 = jnp.float32
THETA = 5.5


def kernel(
    n_lat, n_lon, K, R, C,
    b_hbm, x0_hbm, mask_hbm, ce_hbm, cn_hbm, surf_hbm, w_hbm,
    x_out, r_out,
    stage_w, st_b, st_x0, st_mask, st_ce, st_cn, st_surf,
    ext, zbuf, coef, pack, packs_in, gram_acc, part, red1, red2,
    load_sem, send_sem, recv_sem, s1_send, s1_recv, s2_send, s2_recv,
):
    lat = lax.axis_index("lat")
    lon = lax.axis_index("lon")
    RE = R + 2 * H
    CE = C + 128
    S = 24
    NL = H + 1
    Z = NL * K + 16
    has_n = lat < n_lat - 1
    has_s = lat > 0
    east = lax.rem(lon + 1, n_lon)
    west = lax.rem(lon + n_lon - 1, n_lon)

    loads = []
    pairs = tuple(
        (w_hbm.at[:, pl.ds(128 * t, 128)], stage_w.at[t]) for t in range(C // 128)
    ) + (
        (b_hbm, st_b), (x0_hbm, st_x0), (mask_hbm, st_mask),
        (ce_hbm, st_ce), (cn_hbm, st_cn), (surf_hbm, st_surf),
    )
    for i, (src, dst) in enumerate(pairs):
        c = pltpu.make_async_copy(src, dst, load_sem.at[i])
        c.start()
        loads.append(c)

    barrier = pltpu.get_barrier_semaphore()

    def greet_lat(d, _):
        pl.semaphore_signal(barrier, inc=1, device_id=(lax.rem(lat + d, n_lat), lon), device_id_type=MESH)
        return 0

    def greet_lon(d, _):
        pl.semaphore_signal(barrier, inc=1, device_id=(lat, lax.rem(lon + d, n_lon)), device_id_type=MESH)
        return 0

    lax.fori_loop(1, n_lat, greet_lat, 0)
    lax.fori_loop(1, n_lon, greet_lon, 0)

    @pl.when(has_n)
    def _():
        for t in (east, west):
            pl.semaphore_signal(barrier, inc=1, device_id=(lat + 1, t), device_id_type=MESH)

    @pl.when(has_s)
    def _():
        for t in (east, west):
            pl.semaphore_signal(barrier, inc=1, device_id=(lat - 1, t), device_id_type=MESH)

    for c in loads:
        c.wait()

    for t in range(C // 128):
        ln = pl.ds(128 * t, 128)
        for y in range(R):
            v = stage_w[t, pl.ds(y, K, stride=R), :]
            ext[t, pl.ds(S * y, K), :] = v
            zbuf[t, pl.ds(Z * y, K), :] = v
        fields = (
            st_x0[:, ln], st_b[:, ln], st_mask[:, ln].astype(F32), st_ce[:, ln], st_cn[:, ln], st_surf[:, ln],
        )
        for f, v in enumerate(fields):
            ext[t, pl.ds(K + f, R, stride=S), :] = v
        for f in range(K + 6, S):
            ext[t, pl.ds(f, R, stride=S), :] = jnp.zeros((R, 128), F32)

    lane_s = lax.broadcasted_iota(jnp.int32, (S, 128), 1)
    acc = jnp.zeros((S, 128), F32)
    half = 64
    for y in range(R):
        lo = ext[0, pl.ds(S * y, S), :]
        hi = ext[C // 128 - 1, pl.ds(S * y, S), :]
        a0 = H * y
        if a0:
            lo = pltpu.roll(lo, a0, 1)
        hi = pltpu.roll(hi, (half + a0 + H - 128) % 128, 1)
        acc = jnp.where((lane_s >= a0) & (lane_s < a0 + H), lo, acc)
        acc = jnp.where((lane_s >= half + a0) & (lane_s < half + a0 + H), hi, acc)
    pack[...] = acc

    side = has_n.astype(jnp.int32) + has_s.astype(jnp.int32)
    pl.semaphore_wait(barrier, (n_lat - 1) + (n_lon - 1) + 2 * side)

    own = pl.ds(0, C // 128)

    def copy(src, dst, i, dev):
        return pltpu.make_async_remote_copy(
            src_ref=src, dst_ref=dst, send_sem=send_sem.at[i], recv_sem=recv_sem.at[i],
            device_id=dev, device_id_type=MESH,
        )

    to_n = (
        copy(ext.at[own, pl.ds(S * (R - H), S * H)], ext.at[own, pl.ds(S * (R + H), S * H)], 0, (lat + 1, lon)),
        copy(pack, packs_in.at[2], 4, (lat + 1, east)),
        copy(pack, packs_in.at[3], 5, (lat + 1, west)),
    )
    to_s = (
        copy(ext.at[own, pl.ds(0, S * H)], ext.at[own, pl.ds(S * R, S * H)], 1, (lat - 1, lon)),
        copy(pack, packs_in.at[4], 6, (lat - 1, east)),
        copy(pack, packs_in.at[5], 7, (lat - 1, west)),
    )
    to_e = copy(pack, packs_in.at[0], 2, (lat, east))
    to_w = copy(pack, packs_in.at[1], 3, (lat, west))

    to_e.start()
    to_w.start()

    @pl.when(has_n)
    def _():
        for c in to_n:
            c.start()

    @pl.when(has_s)
    def _():
        for c in to_s:
            c.start()

    to_e.wait()
    to_w.wait()

    def unpack(y_ext, y_src, west_slot, east_slot, keep):
        from_e = packs_in[east_slot]
        from_w = packs_in[west_slot]
        e = pltpu.roll(from_e, (128 - H * y_src) % 128, 1) if y_src else from_e
        w = pltpu.roll(from_w, (128 - H - half - H * y_src) % 128, 1)
        v = jnp.where(lane_s < H, e, jnp.where(lane_s >= 128 - H, w, 0.0))
        if keep is not None:
            v = jnp.where(keep, v, 0.0)
        ext[C // 128, pl.ds(S * y_ext, S), :] = v

    for y in range(R):
        unpack(y, y, 0, 1, None)

    def e_of(v):
        return pltpu.roll(v, CE - 1, 1)

    def w_of(v):
        return pltpu.roll(v, 1, 1)

    def base(n, level):
        def field(f):
            return jnp.concatenate(
                [ext[t, pl.ds(K + f, n, stride=S), :] for t in range(CE // 128)], axis=1
            )

        def n_of(v):
            return pltpu.roll(v, n - 1, 0)

        def s_of(v):
            return pltpu.roll(v, 1, 0)

        x0 = field(0)
        rhs = field(1)
        wet = field(2)
        cew = field(3) * wet
        cnw = field(4) * wet
        k_e = cew * e_of(wet)
        k_w = w_of(cew) * wet
        k_n = cnw * n_of(wet)
        k_s = s_of(cnw) * wet
        centre = field(5) * wet + k_e + k_w + k_n + k_s + (1.0 - wet)
        for i, v in enumerate((centre, k_e, k_w, k_n, k_s)):
            coef[i, 0:n] = v

        def operate(v):
            return centre * v - (k_e * e_of(v) + k_w * w_of(v) + k_n * n_of(v) + k_s * s_of(v))

        s_fam = [rhs - operate(x0)]
        for _ in range(ITERS):
            s_fam.append(operate(s_fam[-1]) - THETA * s_fam[-1])
        for t in range(C // 128):
            for i, v in enumerate(s_fam):
                p = v[:R, 128 * t:128 * t + 128]
                p_hi = p.astype(jnp.bfloat16).astype(F32)
                zbuf[t, pl.ds(NL * K + i, R, stride=Z), :] = p_hi
                zbuf[t, pl.ds(NL * K + 4 + i, R, stride=Z), :] = p - p_hi
            if level == 0:
                for i in range(8, 16):
                    zbuf[t, pl.ds(NL * K + i, R, stride=Z), :] = jnp.zeros((R, 128), F32)

    def rows(level, y):
        y = y % RE
        ref = ext if level == 0 else zbuf
        at = pl.ds(S * y if level == 0 else Z * y + level * K, K)
        return jnp.concatenate([ref[t, at, :] for t in range(CE // 128)], axis=1)

    def step(level, y):
        v = rows(level - 1, y)
        vn = rows(level - 1, y + 1)
        vs = rows(level - 1, y - 1)

        def kk(i):
            return coef[i, pl.ds(y % RE, 1), :]

        diag = kk(0) if level == 1 else kk(0) - THETA
        out = diag * v - (kk(1) * e_of(v) + kk(2) * w_of(v) + kk(3) * vn + kk(4) * vs)
        at = pl.ds(Z * (y % RE) + level * K, K)
        for u in range(CE // 128):
            zbuf[u, at, :] = out[:, 128 * u:128 * u + 128]

    def gram_step(t, total):
        z = jnp.concatenate(
            [
                zbuf[q, pl.ds(pl.multiple_of(Z * (2 * t + u), 8), Z), :]
                for u in range(2) for q in range(C // 128)
            ],
            axis=1,
        )
        hi = z.astype(jnp.bfloat16)
        lo = (z - hi.astype(F32)).astype(jnp.bfloat16)
        both = jnp.concatenate([hi, lo[:NL * K]], axis=0)
        return total + lax.dot_general(
            both, both, (((1,), (1,)), ((), ())), preferred_element_type=F32
        )

    base(R, 0)
    for level in range(1, NL):
        for y in range(level, R - level):
            step(level, y)
    G = jnp.zeros((Z + NL * K, Z + NL * K), F32)
    gram_acc[...] = lax.fori_loop(H // 2, (R - H) // 2, gram_step, G)

    @pl.when(has_n)
    def _():
        for c in to_n:
            c.wait_send()
        for c in to_s:
            c.wait_recv()

    @pl.when(has_s)
    def _():
        for c in to_s:
            c.wait_send()
        for c in to_n:
            c.wait_recv()

    @pl.when(jnp.logical_not(has_n))
    def _():
        ext[:, pl.ds(S * R, S * H), :] = jnp.zeros((CE // 128, S * H, 128), F32)

    @pl.when(jnp.logical_not(has_s))
    def _():
        ext[:, pl.ds(S * (R + H), S * H), :] = jnp.zeros((CE // 128, S * H, 128), F32)

    for y in range(H):
        unpack(R + y, y, 4, 5, has_n)
        unpack(R + H + y, R - H + y, 2, 3, has_s)
    base(RE, 1)
    for level in range(1, NL):
        h = NL - 1 - level
        for y in list(range(-h, level)) + list(range(R - level, R + h)):
            step(level, y)
    G = lax.fori_loop(0, H // 2, gram_step, gram_acc[...])
    G = lax.fori_loop((R - H) // 2, R // 2, gram_step, G)
    zl = jnp.zeros((Z + NL * K, 256 - Z - NL * K), F32)
    G = jnp.concatenate([G, zl], axis=1)
    GL = pltpu.roll(G, 256 - Z, 1)[:, :128]
    G = G[:, :128]

    lane = lax.broadcasted_iota(jnp.int32, (K, 128), 1)
    sub = lax.broadcasted_iota(jnp.int32, (K, 128), 0)

    def moved(v, src, dst):
        s = (dst - src) % 128
        return pltpu.roll(v, s, 1) if s else v

    SB = NL * K
    NM = 2 * ITERS + 1
    AB = NM * K
    P_ = jnp.zeros((K, 128), F32)
    for m in range(1, NM + 1):
        i = m // 2
        j = m - i
        hh = G[i * K:(i + 1) * K] + G[Z + i * K:Z + (i + 1) * K]
        hl = GL[i * K:(i + 1) * K] + GL[Z + i * K:Z + (i + 1) * K]
        dst = (m - 1) * K
        v = moved(hh + hl, j * K, dst)
        P_ = jnp.where((lane >= dst) & (lane < dst + K), v, P_)
    for m in range(NM):
        j = m // 2
        i = m - j
        hh = G[i * K:(i + 1) * K] + G[Z + i * K:Z + (i + 1) * K]
        v = moved(hh, SB + j, AB + m) + moved(hh, SB + 4 + j, AB + m)
        P_ = jnp.where(lane == AB + m, v, P_)
    SL = AB + NM
    for m in range(2 * ITERS):
        i = m // 2
        j = m - i
        g = G[SB:SB + 8]
        v = moved(g, SB + j, SL) + moved(g, SB + 4 + j, SL)
        P_ = jnp.where((lane == SL) & (sub == m), v[i:i + 1] + v[4 + i:5 + i], P_)
    part[...] = P_

    def exchange(src, slots, send, recv, n, me, dev):
        def desc(d):
            return pltpu.make_async_remote_copy(
                src_ref=src, dst_ref=slots.at[me], send_sem=send.at[d], recv_sem=recv.at[me],
                device_id=dev(lax.rem(me + d, n)), device_id_type=MESH,
            )

        def from_slot(d):
            slot = lax.rem(me + d, n)
            return pltpu.make_async_remote_copy(
                src_ref=src, dst_ref=slots.at[slot], send_sem=send.at[d], recv_sem=recv.at[slot],
                device_id=dev(slot), device_id_type=MESH,
            )

        def start(d, _):
            desc(d).start()
            return 0

        def finish(d, _):
            desc(d).wait_send()
            from_slot(d).wait_recv()
            return 0

        lax.fori_loop(1, n, start, 0)
        slots[me] = src[...]
        lax.fori_loop(1, n, finish, 0)
        return lax.fori_loop(0, n, lambda d, t: t + slots[d], jnp.zeros((K, 128), F32))

    part[...] = exchange(part, red1, s1_send, s1_recv, n_lat, lat, lambda o: (o, lon))
    M = exchange(part, red2, s2_send, s2_recv, n_lon, lon, lambda o: (lat, o))

    MT = M.T
    sym = M
    for m in range(NM):
        t = MT[m * K:(m + 1) * K]
        t = jnp.concatenate([t, jnp.zeros((K, 128 - K), F32)], axis=1)
        t = moved(t, 0, m * K)
        sym = jnp.where((lane >= m * K) & (lane < (m + 1) * K), 0.5 * (M + t), sym)

    Q = sym
    for k in range(K):
        column = jnp.broadcast_to(Q[:, k:k + 1], (K, 128))
        pivot = column[k:k + 1]
        unit = (sub == k).astype(F32)
        Q = jnp.where(lane == k, unit, Q)
        Q = Q - (column - unit) * (Q[k:k + 1] / pivot)

    def col(v, m):
        return jnp.sum(jnp.where(lane == (m - 1) * K + sub, v, 0.0), axis=1, keepdims=True)

    def row_of(v):
        return jnp.sum(Q * v, axis=0, keepdims=True)

    def tiled(v):
        return jnp.sum(jnp.where(lax.rem(lane, K) == sub, v, 0.0), axis=0, keepdims=True)

    lane8 = lax.broadcasted_iota(jnp.int32, (8, 128), 1)
    sub8 = lax.broadcasted_iota(jnp.int32, (8, 128), 0)
    seg_mask = lane8 // K == sub8

    def seg_dots(t, v):
        d = jnp.sum(jnp.where(seg_mask, t * v, 0.0), axis=1, keepdims=True)
        return lambda m: d[m - 1:m]

    a = [sym[:, AB + m:AB + m + 1] for m in range(NM)]
    sigma = [M[m:m + 1, SL:SL + 1] for m in range(2 * ITERS)]

    U = row_of(a[0])
    c = col(U, 1)
    cu = seg_dots(tiled(c), U)
    b = [None] + [a[m] - col(U, m + 1) for m in range(1, 4)]
    sg = [sigma[m] - 2.0 * U[:, AB + m + 1:AB + m + 2] + cu(m + 2) for m in range(2 * ITERS)]

    def products(v):
        r = row_of(v)
        q = col(r, 1)
        qt = tiled(q)
        qu = seg_dots(qt, U)
        qb = lambda m: r[:, AB + m:AB + m + 1] - qu(m + 1)
        return r, q, qt, qb

    zero = jnp.zeros((1, 1), F32)

    def norm2(f, gx, gy, gz, e):
        t = gx * gx * q0v(2 + e)
        for i in range(len(f)):
            for k in range(len(f)):
                t = t + f[i] * f[k] * sg[i + k + e]
            t = t + 2.0 * f[i] * gx * q0b(i + 1 + e)
            if gz is not None:
                t = t + 2.0 * f[i] * (gy * q1b(i + 1 + e) + gz * q0b(i + 2 + e))
        if gz is not None:
            t = t + 2.0 * gx * gy * q1v(2 + e) + gy * gy * q1w(2 + e)
            t = t + 2.0 * gz * (gx * q0v(3 + e) + gy * q1v(3 + e)) + gz * gz * q0v(4 + e)
        return t

    V, q0, q0t, q0b = products(b[1])
    q0v = seg_dots(q0t, V)
    v2, v3 = col(V, 2), col(V, 3)
    rn0 = sg[0]
    rz0 = sg[1] + THETA * rn0
    curv0 = rz0 - q0b(1)
    al0 = rn0 / curv0
    f = [1.0 - al0 * THETA, -al0]
    d1 = f[0] * b[1] + f[1] * b[2] + al0 * v2
    Wr, q1, q1t, q1b = products(d1)
    q1v = seg_dots(q1t, V)
    q1w = seg_dots(q1t, Wr)
    w2 = col(Wr, 2)
    rn1 = norm2(f, al0, None, None, 0)
    rz1 = norm2(f, al0, None, None, 1) + THETA * rn1
    be1 = rn1 / rn0
    curv1 = rz1 - jnp.sum(q1 * d1, axis=0, keepdims=True) - be1 * be1 * curv0
    al1 = rn1 / curv1
    gx = al0 - al1 * (THETA * al0 - be1)
    gy = al1
    gz = -al1 * al0
    f = [
        f[0] - al1 * THETA * (f[0] + be1),
        f[1] - al1 * (f[0] + THETA * f[1] + be1),
        -al1 * f[1],
    ]
    d2 = f[0] * b[1] + f[1] * b[2] + f[2] * b[3] + gx * v2 + gy * w2 + gz * v3
    rn2 = norm2(f, gx, gy, gz, 0)
    rz2 = norm2(f, gx, gy, gz, 1) + THETA * rn2
    be2 = rn2 / rn1
    q2 = col(row_of(d2), 1)
    curv2 = rz2 - jnp.sum(q2 * d2, axis=0, keepdims=True) - be2 * be2 * curv1
    al2 = rn2 / curv2

    zc = jnp.zeros((K, 1), F32)

    def combine(x, scale, y):
        n = max(len(x[0]), len(y[0]))
        pad = lambda l, z0, k: list(l) + [z0] * (k - len(l))
        fx, fy = pad(x[0], zero, n), pad(y[0], zero, n)
        m = max(len(x[1]), len(y[1]))
        gx_, gy_ = pad(x[1], zc, m), pad(y[1], zc, m)
        return [p + scale * q for p, q in zip(fx, fy)], [p + scale * q for p, q in zip(gx_, gy_)]

    def shift(x):
        fs = [zero] + x[0]
        gs = [zc] + x[1]
        for i, e in enumerate(x[0]):
            fs[i] = fs[i] + THETA * e
        for i, e in enumerate(x[1]):
            if i:
                gs[i] = gs[i] + THETA * e
        return fs, gs

    one = jnp.ones((1, 1), F32)
    r = ([one], [zc, -c])
    x = ([zero], [c])
    p = combine(r, -one, ([zero], [q0]))
    x = combine(x, al0, p)
    r = combine(r, -al0, shift(p))
    p = combine(combine(r, -one, ([zero], [q1])), be1, p)
    x = combine(x, al1, p)
    r = combine(r, -al1, shift(p))
    p = combine(combine(r, -one, ([zero], [q2])), be2, p)
    x = combine(x, al2, p)
    r = combine(r, -al2, shift(p))

    def column_of(v):
        fs = list(v[0]) + [zero] * (4 - len(v[0]))
        gs = list(v[1]) + [zc] * (NL - len(v[1]))
        s8 = lax.broadcasted_iota(jnp.int32, (16, 128), 0)
        tail = jnp.zeros((16, 128), F32)
        for i, e in enumerate(fs):
            tail = jnp.where((s8 == i) | (s8 == 4 + i), e, tail)
        return [jnp.broadcast_to(g, (K, 128)) for g in gs] + [tail]

    cx = column_of(x)
    cr = column_of(r)
    for y in range(R):
        for t in range(C // 128):
            ln = pl.ds(128 * t, 128)
            tx = jnp.zeros((K, 128), F32)
            tr = jnp.zeros((K, 128), F32)
            for i in range(NL + 1):
                z = zbuf[t, pl.ds(Z * y + i * K, K), :]
                tx = tx + cx[i] * z
                tr = tr + cr[i] * z
            x_out[pl.ds(y, 1), ln] = st_x0[pl.ds(y, 1), ln] + jnp.sum(tx, axis=0, keepdims=True)
            r_out[pl.ds(y, 1), ln] = jnp.sum(tr, axis=0, keepdims=True)


def solution(mesh):
    n_lat, n_lon = mesh.shape["lat"], mesh.shape["lon"]

    def shards(right_side, first_guess, cell_mask, cond_east, cond_north, surface, recycled):
        K, R, C = recycled.shape
        RE, CE, S, Z = R + 2 * H, C + 128, 24, (H + 1) * K + 16
        block = jax.ShapeDtypeStruct((R, C), F32)
        vm = pltpu.VMEM
        dma = pltpu.SemaphoreType.DMA
        return pl.pallas_call(
            functools.partial(kernel, n_lat, n_lon, K, R, C),
            out_shape=(block, block),
            in_specs=[pl.BlockSpec(memory_space=pltpu.HBM)] * 7,
            out_specs=(pl.BlockSpec(memory_space=pltpu.VMEM),) * 2,
            scratch_shapes=[
                vm((C // 128, K * R, 128), F32),
                vm((R, C), F32), vm((R, C), F32), vm((R, C), jnp.int32),
                vm((R, C), F32), vm((R, C), F32), vm((R, C), F32),
                vm((CE // 128, S * RE, 128), F32),
                vm((CE // 128, Z * RE, 128), F32),
                vm((5, RE, CE), F32),
                vm((S, 128), F32),
                vm((6, S, 128), F32),
                vm((Z + (H + 1) * K, Z + (H + 1) * K), F32),
                vm((K, 128), F32),
                vm((n_lat, K, 128), F32),
                vm((n_lon, K, 128), F32),
                dma((6 + C // 128,)), dma((8,)), dma((8,)),
                dma((n_lat,)), dma((n_lat,)), dma((n_lon,)), dma((n_lon,)),
            ],
            compiler_params=pltpu.CompilerParams(
                collective_id=0, has_side_effects=True, vmem_limit_bytes=67043328
            ),
        )(
            right_side, first_guess, cell_mask, cond_east, cond_north, surface,
            recycled.reshape(K * R, C),
        )

    spec = P("lat", "lon")
    return jax.shard_map(
        shards,
        mesh=mesh,
        in_specs=(spec,) * 6 + (P(None, "lat", "lon"),),
        out_specs=(spec, spec),
        check_vma=False,
    )
```

```python
import functools

import jax
import jax.numpy as jnp
from jax import lax
from jax.experimental import pallas as pl
from jax.experimental.pallas import tpu as pltpu
from jax.sharding import PartitionSpec as P

MESH = pl.DeviceIdType.MESH
ITERS = 3
H = 4
F32 = jnp.float32
THETA = 5.5


def kernel(
    n_lat, n_lon, K, R, C,
    b_hbm, x0_hbm, mask_hbm, ce_hbm, cn_hbm, surf_hbm, w_hbm,
    out,
    stage_w, st_b, st_x0, st_mask, st_ce, st_cn, st_surf,
    ext, zbuf, coef, pack, packs_in, gram_acc, part, red1, red2,
    load_sem, send_sem, recv_sem, s1_send, s1_recv, s2_send, s2_recv,
):
    lat = lax.axis_index("lat")
    lon = lax.axis_index("lon")
    RE = R + 2 * H
    CE = C + 128
    S = 24
    NL = H + 1
    Z = NL * K + 16
    has_n = lat < n_lat - 1
    has_s = lat > 0
    east = lax.rem(lon + 1, n_lon)
    west = lax.rem(lon + n_lon - 1, n_lon)

    loads = []
    pairs = tuple(
        (w_hbm.at[:, pl.ds(128 * t, 128)], stage_w.at[t]) for t in range(C // 128)
    ) + (
        (b_hbm, st_b), (x0_hbm, st_x0), (mask_hbm, st_mask),
        (ce_hbm, st_ce), (cn_hbm, st_cn), (surf_hbm, st_surf),
    )
    for i, (src, dst) in enumerate(pairs):
        c = pltpu.make_async_copy(src, dst, load_sem.at[i])
        c.start()
        loads.append(c)

    barrier = pltpu.get_barrier_semaphore()

    def greet_lat(d, _):
        pl.semaphore_signal(barrier, inc=1, device_id=(lax.rem(lat + d, n_lat), lon), device_id_type=MESH)
        return 0

    def greet_lon(d, _):
        pl.semaphore_signal(barrier, inc=1, device_id=(lat, lax.rem(lon + d, n_lon)), device_id_type=MESH)
        return 0

    lax.fori_loop(1, n_lat, greet_lat, 0)
    lax.fori_loop(1, n_lon, greet_lon, 0)

    @pl.when(has_n)
    def _():
        for t in (east, west):
            pl.semaphore_signal(barrier, inc=1, device_id=(lat + 1, t), device_id_type=MESH)

    @pl.when(has_s)
    def _():
        for t in (east, west):
            pl.semaphore_signal(barrier, inc=1, device_id=(lat - 1, t), device_id_type=MESH)

    for c in loads:
        c.wait()

    for t in range(C // 128):
        ln = pl.ds(128 * t, 128)
        for y in range(R):
            v = stage_w[t, pl.ds(y, K, stride=R), :]
            ext[t, pl.ds(S * y, K), :] = v
            zbuf[t, pl.ds(Z * y, K), :] = v
        fields = (
            st_x0[:, ln], st_b[:, ln], st_mask[:, ln].astype(F32), st_ce[:, ln], st_cn[:, ln], st_surf[:, ln],
        )
        for f, v in enumerate(fields):
            ext[t, pl.ds(K + f, R, stride=S), :] = v
        for f in range(K + 6, S):
            ext[t, pl.ds(f, R, stride=S), :] = jnp.zeros((R, 128), F32)

    lane_s = lax.broadcasted_iota(jnp.int32, (S, 128), 1)
    acc = jnp.zeros((S, 128), F32)
    half = 64
    for y in range(R):
        lo = ext[0, pl.ds(S * y, S), :]
        hi = ext[C // 128 - 1, pl.ds(S * y, S), :]
        a0 = H * y
        if a0:
            lo = pltpu.roll(lo, a0, 1)
        hi = pltpu.roll(hi, (half + a0 + H - 128) % 128, 1)
        acc = jnp.where((lane_s >= a0) & (lane_s < a0 + H), lo, acc)
        acc = jnp.where((lane_s >= half + a0) & (lane_s < half + a0 + H), hi, acc)
    pack[...] = acc

    side = has_n.astype(jnp.int32) + has_s.astype(jnp.int32)
    pl.semaphore_wait(barrier, (n_lat - 1) + (n_lon - 1) + 2 * side)

    own = pl.ds(0, C // 128)

    def copy(src, dst, i, dev):
        return pltpu.make_async_remote_copy(
            src_ref=src, dst_ref=dst, send_sem=send_sem.at[i], recv_sem=recv_sem.at[i],
            device_id=dev, device_id_type=MESH,
        )

    to_n = (
        copy(ext.at[own, pl.ds(S * (R - H), S * H)], ext.at[own, pl.ds(S * (R + H), S * H)], 0, (lat + 1, lon)),
        copy(pack, packs_in.at[2], 4, (lat + 1, east)),
        copy(pack, packs_in.at[3], 5, (lat + 1, west)),
    )
    to_s = (
        copy(ext.at[own, pl.ds(0, S * H)], ext.at[own, pl.ds(S * R, S * H)], 1, (lat - 1, lon)),
        copy(pack, packs_in.at[4], 6, (lat - 1, east)),
        copy(pack, packs_in.at[5], 7, (lat - 1, west)),
    )
    to_e = copy(pack, packs_in.at[0], 2, (lat, east))
    to_w = copy(pack, packs_in.at[1], 3, (lat, west))

    to_e.start()
    to_w.start()

    @pl.when(has_n)
    def _():
        for c in to_n:
            c.start()

    @pl.when(has_s)
    def _():
        for c in to_s:
            c.start()

    to_e.wait()
    to_w.wait()

    def unpack(y_ext, y_src, west_slot, east_slot, keep):
        from_e = packs_in[east_slot]
        from_w = packs_in[west_slot]
        e = pltpu.roll(from_e, (128 - H * y_src) % 128, 1) if y_src else from_e
        w = pltpu.roll(from_w, (128 - H - half - H * y_src) % 128, 1)
        v = jnp.where(lane_s < H, e, jnp.where(lane_s >= 128 - H, w, 0.0))
        if keep is not None:
            v = jnp.where(keep, v, 0.0)
        ext[C // 128, pl.ds(S * y_ext, S), :] = v

    for y in range(R):
        unpack(y, y, 0, 1, None)

    def e_of(v):
        return pltpu.roll(v, CE - 1, 1)

    def w_of(v):
        return pltpu.roll(v, 1, 1)

    def base(n, level):
        def field(f):
            return jnp.concatenate(
                [ext[t, pl.ds(K + f, n, stride=S), :] for t in range(CE // 128)], axis=1
            )

        def n_of(v):
            return pltpu.roll(v, n - 1, 0)

        def s_of(v):
            return pltpu.roll(v, 1, 0)

        x0 = field(0)
        rhs = field(1)
        wet = field(2)
        cew = field(3) * wet
        cnw = field(4) * wet
        k_e = cew * e_of(wet)
        k_w = w_of(cew) * wet
        k_n = cnw * n_of(wet)
        k_s = s_of(cnw) * wet
        centre = field(5) * wet + k_e + k_w + k_n + k_s + (1.0 - wet)
        for i, v in enumerate((centre, k_e, k_w, k_n, k_s)):
            coef[i, 0:n] = v

        def operate(v):
            return centre * v - (k_e * e_of(v) + k_w * w_of(v) + k_n * n_of(v) + k_s * s_of(v))

        s_fam = [rhs - operate(x0)]
        for _ in range(ITERS):
            s_fam.append(operate(s_fam[-1]) - THETA * s_fam[-1])
        for t in range(C // 128):
            for i, v in enumerate(s_fam):
                p = v[:R, 128 * t:128 * t + 128]
                p_hi = p.astype(jnp.bfloat16).astype(F32)
                zbuf[t, pl.ds(NL * K + i, R, stride=Z), :] = p_hi
                zbuf[t, pl.ds(NL * K + 4 + i, R, stride=Z), :] = p - p_hi
            if level == 0:
                for i in range(8, 16):
                    zbuf[t, pl.ds(NL * K + i, R, stride=Z), :] = jnp.zeros((R, 128), F32)

    def rows(level, y):
        y = y % RE
        ref = ext if level == 0 else zbuf
        at = pl.ds(S * y if level == 0 else Z * y + level * K, K)
        return jnp.concatenate([ref[t, at, :] for t in range(CE // 128)], axis=1)

    def step(level, y):
        v = rows(level - 1, y)
        vn = rows(level - 1, y + 1)
        vs = rows(level - 1, y - 1)

        def kk(i):
            return coef[i, pl.ds(y % RE, 1), :]

        diag = kk(0) if level == 1 else kk(0) - THETA
        out = diag * v - (kk(1) * e_of(v) + kk(2) * w_of(v) + kk(3) * vn + kk(4) * vs)
        at = pl.ds(Z * (y % RE) + level * K, K)
        for u in range(CE // 128):
            zbuf[u, at, :] = out[:, 128 * u:128 * u + 128]

    def gram_step(t, total):
        z = jnp.concatenate(
            [
                zbuf[q, pl.ds(pl.multiple_of(Z * (2 * t + u), 8), Z), :]
                for u in range(2) for q in range(C // 128)
            ],
            axis=1,
        )
        hi = z.astype(jnp.bfloat16)
        lo = (z - hi.astype(F32)).astype(jnp.bfloat16)
        both = jnp.concatenate([hi, lo[:NL * K]], axis=0)
        return total + lax.dot_general(
            both, both, (((1,), (1,)), ((), ())), preferred_element_type=F32
        )

    base(R, 0)
    for level in range(1, NL):
        for y in range(level, R - level):
            step(level, y)
    G = jnp.zeros((Z + NL * K, Z + NL * K), F32)
    gram_acc[...] = lax.fori_loop(H // 2, (R - H) // 2, gram_step, G)

    @pl.when(has_n)
    def _():
        for c in to_n:
            c.wait_send()
        for c in to_s:
            c.wait_recv()

    @pl.when(has_s)
    def _():
        for c in to_s:
            c.wait_send()
        for c in to_n:
            c.wait_recv()

    @pl.when(jnp.logical_not(has_n))
    def _():
        ext[:, pl.ds(S * R, S * H), :] = jnp.zeros((CE // 128, S * H, 128), F32)

    @pl.when(jnp.logical_not(has_s))
    def _():
        ext[:, pl.ds(S * (R + H), S * H), :] = jnp.zeros((CE // 128, S * H, 128), F32)

    for y in range(H):
        unpack(R + y, y, 4, 5, has_n)
        unpack(R + H + y, R - H + y, 2, 3, has_s)
    base(RE, 1)
    for level in range(1, NL):
        h = NL - 1 - level
        for y in list(range(-h, level)) + list(range(R - level, R + h)):
            step(level, y)
    G = lax.fori_loop(0, H // 2, gram_step, gram_acc[...])
    G = lax.fori_loop((R - H) // 2, R // 2, gram_step, G)
    zl = jnp.zeros((Z + NL * K, 256 - Z - NL * K), F32)
    G = jnp.concatenate([G, zl], axis=1)
    GL = pltpu.roll(G, 256 - Z, 1)[:, :128]
    G = G[:, :128]

    lane = lax.broadcasted_iota(jnp.int32, (K, 128), 1)
    sub = lax.broadcasted_iota(jnp.int32, (K, 128), 0)

    def moved(v, src, dst):
        s = (dst - src) % 128
        return pltpu.roll(v, s, 1) if s else v

    SB = NL * K
    NM = 2 * ITERS + 1
    AB = NM * K
    P_ = jnp.zeros((K, 128), F32)
    for m in range(1, NM + 1):
        i = m // 2
        j = m - i
        hh = G[i * K:(i + 1) * K] + G[Z + i * K:Z + (i + 1) * K]
        hl = GL[i * K:(i + 1) * K] + GL[Z + i * K:Z + (i + 1) * K]
        dst = (m - 1) * K
        v = moved(hh + hl, j * K, dst)
        P_ = jnp.where((lane >= dst) & (lane < dst + K), v, P_)
    for m in range(NM):
        j = m // 2
        i = m - j
        hh = G[i * K:(i + 1) * K] + G[Z + i * K:Z + (i + 1) * K]
        v = moved(hh, SB + j, AB + m) + moved(hh, SB + 4 + j, AB + m)
        P_ = jnp.where(lane == AB + m, v, P_)
    SL = AB + NM
    for m in range(2 * ITERS):
        i = m // 2
        j = m - i
        g = G[SB:SB + 8]
        v = moved(g, SB + j, SL) + moved(g, SB + 4 + j, SL)
        P_ = jnp.where((lane == SL) & (sub == m), v[i:i + 1] + v[4 + i:5 + i], P_)
    part[...] = P_

    def exchange(src, slots, send, recv, n, me, dev):
        def desc(d):
            return pltpu.make_async_remote_copy(
                src_ref=src, dst_ref=slots.at[me], send_sem=send.at[d], recv_sem=recv.at[me],
                device_id=dev(lax.rem(me + d, n)), device_id_type=MESH,
            )

        def from_slot(d):
            slot = lax.rem(me + d, n)
            return pltpu.make_async_remote_copy(
                src_ref=src, dst_ref=slots.at[slot], send_sem=send.at[d], recv_sem=recv.at[slot],
                device_id=dev(slot), device_id_type=MESH,
            )

        def start(d, _):
            desc(d).start()
            return 0

        def finish(d, _):
            desc(d).wait_send()
            from_slot(d).wait_recv()
            return 0

        lax.fori_loop(1, n, start, 0)
        slots[me] = src[...]
        lax.fori_loop(1, n, finish, 0)
        return lax.fori_loop(0, n, lambda d, t: t + slots[d], jnp.zeros((K, 128), F32))

    part[...] = exchange(part, red1, s1_send, s1_recv, n_lat, lat, lambda o: (o, lon))
    M = exchange(part, red2, s2_send, s2_recv, n_lon, lon, lambda o: (lat, o))

    MT = M.T
    sym = M
    for m in range(NM):
        t = MT[m * K:(m + 1) * K]
        t = jnp.concatenate([t, jnp.zeros((K, 128 - K), F32)], axis=1)
        t = moved(t, 0, m * K)
        sym = jnp.where((lane >= m * K) & (lane < (m + 1) * K), 0.5 * (M + t), sym)

    Q = sym
    for k in range(K):
        column = jnp.broadcast_to(Q[:, k:k + 1], (K, 128))
        pivot = column[k:k + 1]
        unit = (sub == k).astype(F32)
        Q = jnp.where(lane == k, unit, Q)
        Q = Q - (column - unit) * (Q[k:k + 1] / pivot)

    def col(v, m):
        return jnp.sum(jnp.where(lane == (m - 1) * K + sub, v, 0.0), axis=1, keepdims=True)

    def row_of(v):
        return jnp.sum(Q * v, axis=0, keepdims=True)

    def tiled(v):
        return jnp.sum(jnp.where(lax.rem(lane, K) == sub, v, 0.0), axis=0, keepdims=True)

    lane8 = lax.broadcasted_iota(jnp.int32, (8, 128), 1)
    sub8 = lax.broadcasted_iota(jnp.int32, (8, 128), 0)
    seg_mask = lane8 // K == sub8

    def seg_dots(t, v):
        d = jnp.sum(jnp.where(seg_mask, t * v, 0.0), axis=1, keepdims=True)
        return lambda m: d[m - 1:m]

    a = [sym[:, AB + m:AB + m + 1] for m in range(NM)]
    sigma = [M[m:m + 1, SL:SL + 1] for m in range(2 * ITERS)]

    U = row_of(a[0])
    c = col(U, 1)
    cu = seg_dots(tiled(c), U)
    b = [None] + [a[m] - col(U, m + 1) for m in range(1, 4)]
    sg = [sigma[m] - 2.0 * U[:, AB + m + 1:AB + m + 2] + cu(m + 2) for m in range(2 * ITERS)]

    def products(v):
        r = row_of(v)
        q = col(r, 1)
        qt = tiled(q)
        qu = seg_dots(qt, U)
        qb = lambda m: r[:, AB + m:AB + m + 1] - qu(m + 1)
        return r, q, qt, qb

    zero = jnp.zeros((1, 1), F32)

    def norm2(f, gx, gy, gz, e):
        t = gx * gx * q0v(2 + e)
        for i in range(len(f)):
            for k in range(len(f)):
                t = t + f[i] * f[k] * sg[i + k + e]
            t = t + 2.0 * f[i] * gx * q0b(i + 1 + e)
            if gz is not None:
                t = t + 2.0 * f[i] * (gy * q1b(i + 1 + e) + gz * q0b(i + 2 + e))
        if gz is not None:
            t = t + 2.0 * gx * gy * q1v(2 + e) + gy * gy * q1w(2 + e)
            t = t + 2.0 * gz * (gx * q0v(3 + e) + gy * q1v(3 + e)) + gz * gz * q0v(4 + e)
        return t

    V, q0, q0t, q0b = products(b[1])
    q0v = seg_dots(q0t, V)
    v2, v3 = col(V, 2), col(V, 3)
    rn0 = sg[0]
    rz0 = sg[1] + THETA * rn0
    curv0 = rz0 - q0b(1)
    al0 = rn0 / curv0
    f = [1.0 - al0 * THETA, -al0]
    d1 = f[0] * b[1] + f[1] * b[2] + al0 * v2
    Wr, q1, q1t, q1b = products(d1)
    q1v = seg_dots(q1t, V)
    q1w = seg_dots(q1t, Wr)
    w2 = col(Wr, 2)
    rn1 = norm2(f, al0, None, None, 0)
    rz1 = norm2(f, al0, None, None, 1) + THETA * rn1
    be1 = rn1 / rn0
    curv1 = rz1 - jnp.sum(q1 * d1, axis=0, keepdims=True) - be1 * be1 * curv0
    al1 = rn1 / curv1
    gx = al0 - al1 * (THETA * al0 - be1)
    gy = al1
    gz = -al1 * al0
    f = [
        f[0] - al1 * THETA * (f[0] + be1),
        f[1] - al1 * (f[0] + THETA * f[1] + be1),
        -al1 * f[1],
    ]
    d2 = f[0] * b[1] + f[1] * b[2] + f[2] * b[3] + gx * v2 + gy * w2 + gz * v3
    rn2 = norm2(f, gx, gy, gz, 0)
    rz2 = norm2(f, gx, gy, gz, 1) + THETA * rn2
    be2 = rn2 / rn1
    q2 = col(row_of(d2), 1)
    curv2 = rz2 - jnp.sum(q2 * d2, axis=0, keepdims=True) - be2 * be2 * curv1
    al2 = rn2 / curv2

    zc = jnp.zeros((K, 1), F32)

    def combine(x, scale, y):
        n = max(len(x[0]), len(y[0]))
        pad = lambda l, z0, k: list(l) + [z0] * (k - len(l))
        fx, fy = pad(x[0], zero, n), pad(y[0], zero, n)
        m = max(len(x[1]), len(y[1]))
        gx_, gy_ = pad(x[1], zc, m), pad(y[1], zc, m)
        return [p + scale * q for p, q in zip(fx, fy)], [p + scale * q for p, q in zip(gx_, gy_)]

    def shift(x):
        fs = [zero] + x[0]
        gs = [zc] + x[1]
        for i, e in enumerate(x[0]):
            fs[i] = fs[i] + THETA * e
        for i, e in enumerate(x[1]):
            if i:
                gs[i] = gs[i] + THETA * e
        return fs, gs

    one = jnp.ones((1, 1), F32)
    r = ([one], [zc, -c])
    x = ([zero], [c])
    p = combine(r, -one, ([zero], [q0]))
    x = combine(x, al0, p)
    r = combine(r, -al0, shift(p))
    p = combine(combine(r, -one, ([zero], [q1])), be1, p)
    x = combine(x, al1, p)
    r = combine(r, -al1, shift(p))
    p = combine(combine(r, -one, ([zero], [q2])), be2, p)
    x = combine(x, al2, p)
    r = combine(r, -al2, shift(p))

    def column_of(v):
        fs = list(v[0]) + [zero] * (4 - len(v[0]))
        gs = list(v[1]) + [zc] * (NL - len(v[1]))
        s8 = lax.broadcasted_iota(jnp.int32, (16, 128), 0)
        tail = jnp.zeros((16, 128), F32)
        for i, e in enumerate(fs):
            tail = jnp.where((s8 == i) | (s8 == 4 + i), e, tail)
        return [jnp.broadcast_to(g, (K, 128)) for g in gs] + [tail]

    cx = column_of(x)
    cr = column_of(r)
    for y in range(R):
        for t in range(C // 128):
            ln = pl.ds(128 * t, 128)
            tx = jnp.zeros((K, 128), F32)
            tr = jnp.zeros((K, 128), F32)
            for i in range(NL + 1):
                z = zbuf[t, pl.ds(Z * y + i * K, K), :]
                tx = tx + cx[i] * z
                tr = tr + cr[i] * z
            out[pl.ds(y, 1), ln] = st_x0[pl.ds(y, 1), ln] + jnp.sum(tx, axis=0, keepdims=True)
            out[pl.ds(R + y, 1), ln] = jnp.sum(tr, axis=0, keepdims=True)


def solution(mesh):
    n_lat, n_lon = mesh.shape["lat"], mesh.shape["lon"]

    def shards(right_side, first_guess, cell_mask, cond_east, cond_north, surface, recycled):
        K, R, C = recycled.shape
        RE, CE, S, Z = R + 2 * H, C + 128, 24, (H + 1) * K + 16
        block = jax.ShapeDtypeStruct((2 * R, C), F32)
        vm = pltpu.VMEM
        dma = pltpu.SemaphoreType.DMA
        both = pl.pallas_call(
            functools.partial(kernel, n_lat, n_lon, K, R, C),
            out_shape=block,
            in_specs=[pl.BlockSpec(memory_space=pltpu.HBM)] * 7,
            out_specs=pl.BlockSpec(memory_space=pltpu.VMEM),
            scratch_shapes=[
                vm((C // 128, K * R, 128), F32),
                vm((R, C), F32), vm((R, C), F32), vm((R, C), jnp.int32),
                vm((R, C), F32), vm((R, C), F32), vm((R, C), F32),
                vm((CE // 128, S * RE, 128), F32),
                vm((CE // 128, Z * RE, 128), F32),
                vm((5, RE, CE), F32),
                vm((S, 128), F32),
                vm((6, S, 128), F32),
                vm((Z + (H + 1) * K, Z + (H + 1) * K), F32),
                vm((K, 128), F32),
                vm((n_lat, K, 128), F32),
                vm((n_lon, K, 128), F32),
                dma((6 + C // 128,)), dma((8,)), dma((8,)),
                dma((n_lat,)), dma((n_lat,)), dma((n_lon,)), dma((n_lon,)),
            ],
            compiler_params=pltpu.CompilerParams(
                collective_id=0, has_side_effects=True, vmem_limit_bytes=67043328
            ),
        )(
            right_side, first_guess, cell_mask, cond_east, cond_north, surface,
            recycled.reshape(K * R, C),
        )
        return both[:R], both[R:]

    spec = P("lat", "lon")
    return jax.shard_map(
        shards,
        mesh=mesh,
        in_specs=(spec,) * 6 + (P(None, "lat", "lon"),),
        out_specs=(spec, spec),
        check_vma=False,
    )
```
